16 devices in a mesh: dp: 2 (over z), tp: 8 (over y, x, core).
Axes of the slice: x: 2, y: 2, z: 2, core: 2. Of those that a mesh axis runs over, the one named last changes fastest.
Arguments:
- layer_in: bfloat16 [32, 256, 4096], P('dp', 'tp'), parts along dimension 0
- grad_out: bfloat16 [32, 256, 4096], P('dp', 'tp'), parts along dimension 0
- w_qkv: bfloat16 [4096, 32, 3, 128], P(None, 'tp')
- w_out: bfloat16 [32, 1, 128, 4096], P('tp')
- w_up: bfloat16 [4096, 16384], P(None, 'tp')
- w_down: bfloat16 [16384, 4096], P('tp')
- ln_params: float32 [4, 4096], replicated
Outputs:
- output 1: bfloat16 [32, 256, 4096], P('dp', 'tp'), parts along dimension 0
- output 2: bfloat16 [8192, 32, 3, 128], P('dp', 'tp'), parts along dimension 0
- output 3: bfloat16 [64, 1, 128, 4096], P(('dp', 'tp')), parts along dimension 0
- output 4: bfloat16 [8192, 16384], P('dp', 'tp'), parts along dimension 0
- output 5: bfloat16 [32768, 4096], P(('dp', 'tp')), parts along dimension 0
- output 6: float32 [8, 4096], P('dp'), parts along dimension 0
There are 2 independent parts. The reference program is written for one: setup_inputs(seed, part) draws one part's arguments, and reference() takes and returns one part's arrays. A program takes and returns all parts, laid end to end along the dimension named above; an argument that names none is the same for every part.
All inputs are finite; a program needn't handle non-finite values.
Results may differ from the reference program's by a relative error of at most 0.0074571.
Values are sent between devices in bfloat16 or wider.
A program may use at most 1 GiB of HBM per device.

```python
import jax
import jax.numpy as jnp
from jax import lax

D = 4096
HEADS = 32
KV_HEADS = 32
HEAD = 128
FF = 16384
BATCH = 16
SEQ = 256

NORM_EPS = 1e-5
ROPE_BASE = 10000.0
NEG_BIG = -1e30


def setup_inputs(seed: int = 0, part: int = 0) -> dict:
    part_key = jax.random.fold_in(jax.random.key(seed), part)
    key_in, key_grad = jax.random.split(part_key, 2)
    key_qkv, key_out, key_up, key_down, key_norm = jax.random.split(jax.random.key(seed + 1), 5)
    group_size = HEADS // KV_HEADS
    layer_in = jax.random.normal(key_in, (BATCH, SEQ, D), jnp.float32).astype(jnp.bfloat16)
    grad_out = jax.random.normal(key_grad, (BATCH, SEQ, D), jnp.float32).astype(jnp.bfloat16)
    w_qkv = (jax.random.normal(key_qkv, (D, KV_HEADS, group_size + 2, HEAD), jnp.float32) * D ** -0.5).astype(jnp.bfloat16)
    w_out = (jax.random.normal(key_out, (KV_HEADS, group_size, HEAD, D), jnp.float32) * (HEADS * HEAD) ** -0.5).astype(jnp.bfloat16)
    w_up = (jax.random.normal(key_up, (D, FF), jnp.float32) * D ** -0.5).astype(jnp.bfloat16)
    w_down = (jax.random.normal(key_down, (FF, D), jnp.float32) * FF ** -0.5).astype(jnp.bfloat16)
    centre = jnp.array([1.0, 0.0, 1.0, 0.0], jnp.float32)
    ln_params = centre[:, None] + 0.25 * jax.random.normal(key_norm, (4, D), jnp.float32)
    return {'layer_in': layer_in, 'grad_out': grad_out, 'w_qkv': w_qkv, 'w_out': w_out, 'w_up': w_up, 'w_down': w_down, 'ln_params': ln_params}


def norm_stats(source):
    widened = source.astype(jnp.float32)
    centred = widened - jnp.mean(widened, axis=-1, keepdims=True)
    inv_std = lax.rsqrt(jnp.mean(centred * centred, axis=-1, keepdims=True) + NORM_EPS)
    return centred * inv_std, inv_std


def norm_backward(cotangent, normed, inv_std, gain_row):
    scaled = cotangent * gain_row
    return inv_std * (scaled - jnp.mean(scaled, axis=-1, keepdims=True) - normed * jnp.mean(scaled * normed, axis=-1, keepdims=True))


def rope_tables(seq_len, head_dim):
    half_dim = head_dim // 2
    inv_freq = ROPE_BASE ** (-2.0 * jnp.arange(half_dim, dtype=jnp.float32) / head_dim)
    angles = jnp.arange(seq_len, dtype=jnp.float32)[:, None] * inv_freq[None, :]
    angles = jnp.concatenate([angles, angles], axis=-1)
    return jnp.cos(angles), jnp.sin(angles)


def rotate_half(tensor):
    half_dim = tensor.shape[-1] // 2
    return jnp.concatenate([-tensor[..., half_dim:], tensor[..., :half_dim]], axis=-1)


def rotate_half_back(tensor):
    half_dim = tensor.shape[-1] // 2
    return jnp.concatenate([tensor[..., half_dim:], -tensor[..., :half_dim]], axis=-1)


def apply_rope(tensor, cos_tab, sin_tab):
    widened = tensor.astype(jnp.float32)
    return (widened * cos_tab + rotate_half(widened) * sin_tab).astype(jnp.bfloat16)


def rope_backward(cotangent, cos_tab, sin_tab):
    return cotangent * cos_tab + rotate_half_back(cotangent * sin_tab)


def exact_gelu(pre_vals):
    return jax.nn.gelu(pre_vals, approximate=False)


def group_attention(operands):
    queries, key_rot, val_rows, ctx_grad = operands
    seq_len = queries.shape[1]
    score_scale = queries.shape[-1] ** -0.5
    positions = jnp.arange(seq_len)
    causal = positions[:, None] >= positions[None, :]
    scores = jnp.einsum('bqjh,bkh->bjqk', queries.astype(jnp.float32), key_rot.astype(jnp.float32)) * score_scale
    scores = jnp.where(causal, scores, NEG_BIG)
    attn_probs = jax.nn.softmax(scores, axis=-1)
    probs_bf16 = attn_probs.astype(jnp.bfloat16).astype(jnp.float32)
    context = jnp.einsum('bjqk,bkh->bqjh', probs_bf16, val_rows.astype(jnp.float32)).astype(jnp.bfloat16)
    prob_grad = jnp.einsum('bqjh,bkh->bjqk', ctx_grad.astype(jnp.float32), val_rows.astype(jnp.float32))
    val_grad = jnp.einsum('bjqk,bqjh->bkh', probs_bf16, ctx_grad.astype(jnp.float32))
    score_grad = attn_probs * (prob_grad - jnp.sum(prob_grad * attn_probs, axis=-1, keepdims=True))
    score_grad = (score_grad * score_scale).astype(jnp.bfloat16).astype(jnp.float32)
    query_grad = jnp.einsum('bjqk,bkh->bqjh', score_grad, key_rot.astype(jnp.float32))
    key_grad = jnp.einsum('bjqk,bqjh->bkh', score_grad, queries.astype(jnp.float32))
    return context, query_grad, key_grad, val_grad


def reference(layer_in, grad_out, w_qkv, w_out, w_up, w_down, ln_params):
    group_size = HEADS // KV_HEADS
    row_count = BATCH * SEQ
    normed, inv_std = norm_stats(layer_in.reshape(row_count, D))
    attn_in = (normed * ln_params[0] + ln_params[1]).astype(jnp.bfloat16)
    mlp_in = (normed * ln_params[2] + ln_params[3]).astype(jnp.bfloat16)
    qkv_flat = w_qkv.reshape(D, KV_HEADS * (group_size + 2) * HEAD)
    proj_qkv = jnp.dot(attn_in, qkv_flat, preferred_element_type=jnp.float32).astype(jnp.bfloat16)
    proj_qkv = proj_qkv.reshape(BATCH, SEQ, KV_HEADS, group_size + 2, HEAD)
    cos_tab, sin_tab = rope_tables(SEQ, HEAD)
    cos_q = cos_tab[:, None, None, :]
    sin_q = sin_tab[:, None, None, :]
    cos_k = cos_tab[:, None, :]
    sin_k = sin_tab[:, None, :]
    queries = apply_rope(proj_qkv[:, :, :, :group_size], cos_q, sin_q)
    key_rot = apply_rope(proj_qkv[:, :, :, group_size], cos_k, sin_k)
    val_rows = proj_qkv[:, :, :, group_size + 1]
    grad_rows = grad_out.reshape(row_count, D)
    out_flat = w_out.reshape(HEADS * HEAD, D)
    ctx_grad = jnp.dot(grad_rows, out_flat.T, preferred_element_type=jnp.float32).astype(jnp.bfloat16)
    ctx_grad = ctx_grad.reshape(BATCH, SEQ, KV_HEADS, group_size, HEAD)
    by_group = (jnp.moveaxis(queries, 2, 0), jnp.moveaxis(key_rot, 2, 0), jnp.moveaxis(val_rows, 2, 0), jnp.moveaxis(ctx_grad, 2, 0))
    context, query_grad, key_grad, val_grad = lax.map(group_attention, by_group)
    context = jnp.moveaxis(context, 0, 2)
    query_grad = rope_backward(jnp.moveaxis(query_grad, 0, 2), cos_q, sin_q)
    key_grad = rope_backward(jnp.moveaxis(key_grad, 0, 2), cos_k, sin_k)
    val_grad = jnp.moveaxis(val_grad, 0, 2)
    qkv_grad = jnp.concatenate([query_grad, key_grad[:, :, :, None], val_grad[:, :, :, None]], axis=3)
    qkv_grad = qkv_grad.astype(jnp.bfloat16).reshape(row_count, KV_HEADS * (group_size + 2) * HEAD)
    attn_cot = jnp.dot(qkv_grad, qkv_flat.T, preferred_element_type=jnp.float32)
    grad_qkv = jnp.dot(attn_in.T, qkv_grad, preferred_element_type=jnp.float32).astype(jnp.bfloat16).reshape(w_qkv.shape)
    grad_wout = jnp.dot(context.reshape(row_count, HEADS * HEAD).T, grad_rows, preferred_element_type=jnp.float32).astype(jnp.bfloat16).reshape(w_out.shape)
    pre_act = jnp.dot(mlp_in, w_up, preferred_element_type=jnp.float32)
    act_vals, gelu_vjp = jax.vjp(exact_gelu, pre_act)
    act_grad = jnp.dot(grad_rows, w_down.T, preferred_element_type=jnp.float32)
    hidden_grad = gelu_vjp(act_grad)[0].astype(jnp.bfloat16)
    grad_down = jnp.dot(act_vals.astype(jnp.bfloat16).T, grad_rows, preferred_element_type=jnp.float32).astype(jnp.bfloat16)
    grad_up = jnp.dot(mlp_in.T, hidden_grad, preferred_element_type=jnp.float32).astype(jnp.bfloat16)
    mlp_cot = jnp.dot(hidden_grad, w_up.T, preferred_element_type=jnp.float32)
    grad_in = grad_rows.astype(jnp.float32) + norm_backward(attn_cot, normed, inv_std, ln_params[0]) + norm_backward(mlp_cot, normed, inv_std, ln_params[2])
    grad_ln = jnp.stack([jnp.sum(attn_cot * normed, axis=0), jnp.sum(attn_cot, axis=0), jnp.sum(mlp_cot * normed, axis=0), jnp.sum(mlp_cot, axis=0)])
    return (grad_in.astype(jnp.bfloat16).reshape(BATCH, SEQ, D), grad_qkv, grad_wout, grad_up, grad_down, grad_ln)
```

```python
import functools
import math

import jax
import jax.numpy as jnp
from jax import lax
from jax.experimental import pallas as pl
from jax.experimental.pallas import tpu as pltpu
from jax.sharding import PartitionSpec as P


NORM_EPS = 1e-5
ROPE_BASE = 10000.0
NEG_BIG = -1e30
SIZES = (4, 6, 6)
VMEM = 62 * 1024 * 1024
F32 = jnp.float32
BF16 = jnp.bfloat16


def dot(lhs, rhs, lc, rc):
    return lax.dot_general(lhs, rhs, (((lc,), (rc,)), ((), ())), preferred_element_type=F32)


def rope_tables(seq_len, head_dim):
    half_dim = head_dim // 2
    inv_freq = ROPE_BASE ** (-2.0 * jnp.arange(half_dim, dtype=F32) / head_dim)
    angles = jnp.arange(seq_len, dtype=F32)[:, None] * inv_freq[None, :]
    sin = jnp.sin(angles)
    cos = jnp.cos(angles)
    return jnp.concatenate([cos, cos], axis=-1), jnp.concatenate([-sin, sin], axis=-1)


def attention_kernel(heads, head_dim, qkv_ref, dc_ref, cos_ref, sin_ref, c_ref, dqkv_ref):
    seq = qkv_ref.shape[1]
    half = head_dim // 2
    width = heads * head_dim
    scale = head_dim ** -0.5
    cos = cos_ref[...]
    sin = sin_ref[...]
    causal = lax.broadcasted_iota(jnp.int32, (seq, seq), 0) >= lax.broadcasted_iota(jnp.int32, (seq, seq), 1)
    for h in range(heads):
        cols = slice(h * head_dim, (h + 1) * head_dim)
        k_cols = slice(width + h * head_dim, width + (h + 1) * head_dim)
        v_cols = slice(2 * width + h * head_dim, 2 * width + (h + 1) * head_dim)
        q = qkv_ref[0, :, cols].astype(F32)
        k = qkv_ref[0, :, k_cols].astype(F32)
        v = qkv_ref[0, :, v_cols]
        dc = dc_ref[0, :, cols]
        q2 = (q * cos + pltpu.roll(q, half, 1) * sin).astype(BF16)
        k2 = (k * cos + pltpu.roll(k, half, 1) * sin).astype(BF16)
        scores = dot(q2, k2, 1, 1) * scale
        scores = jnp.where(causal, scores, NEG_BIG)
        weights = jnp.exp(scores - jnp.max(scores, axis=-1, keepdims=True))
        probs = weights / jnp.sum(weights, axis=-1, keepdims=True)
        probs_bf16 = probs.astype(BF16)
        c_ref[0, :, cols] = dot(probs_bf16, v, 1, 0).astype(BF16)
        dpr = dot(dc, v, 1, 1)
        ds = probs * (dpr - jnp.sum(dpr * probs, axis=-1, keepdims=True))
        ds = (ds * scale).astype(BF16)
        dq2 = dot(ds, k2, 1, 0)
        dk2 = dot(ds, q2, 0, 0)
        dv = dot(probs_bf16, dc, 0, 0)
        dqkv_ref[0, :, cols] = (dq2 * cos - pltpu.roll(dq2, half, 1) * sin).astype(BF16)
        dqkv_ref[0, :, k_cols] = (dk2 * cos - pltpu.roll(dk2, half, 1) * sin).astype(BF16)
        dqkv_ref[0, :, v_cols] = dv.astype(BF16)


def attention_grads(qkv, dc, cos, sin, head_dim):
    batch, seq, qkv_width = qkv.shape
    width = qkv_width // 3
    heads = width // head_dim
    flops = batch * heads * 6 * 2 * seq * seq * head_dim
    return pl.pallas_call(
        functools.partial(attention_kernel, heads, head_dim),
        grid=(batch,),
        in_specs=[
            pl.BlockSpec((1, seq, qkv_width), lambda b: (b, 0, 0)),
            pl.BlockSpec((1, seq, width), lambda b: (b, 0, 0)),
            pl.BlockSpec((seq, head_dim), lambda b: (0, 0)),
            pl.BlockSpec((seq, head_dim), lambda b: (0, 0)),
        ],
        out_specs=[
            pl.BlockSpec((1, seq, width), lambda b: (b, 0, 0)),
            pl.BlockSpec((1, seq, qkv_width), lambda b: (b, 0, 0)),
        ],
        out_shape=[jax.ShapeDtypeStruct((batch, seq, width), BF16), jax.ShapeDtypeStruct(qkv.shape, BF16)],
        cost_estimate=pl.CostEstimate(flops=flops * 3, bytes_accessed=batch * seq * width * 16, transcendentals=batch * heads * seq * seq),
        name="attention_grads",
    )(qkv, dc, cos, sin)


def params_for(**kw):
    return pltpu.CompilerParams(vmem_limit_bytes=VMEM, **kw)


def norm_kernel(x_ref, par_ref, a_ref, m_ref, mean_ref, rstd_ref):
    x = x_ref[...].astype(F32)
    mean = jnp.mean(x, axis=-1, keepdims=True)
    centred = x - mean
    rstd = lax.rsqrt(jnp.mean(centred * centred, axis=-1, keepdims=True) + NORM_EPS)
    xh = centred * rstd
    a_ref[...] = (xh * par_ref[0:1, :] + par_ref[1:2, :]).astype(BF16)
    m_ref[...] = (xh * par_ref[2:3, :] + par_ref[3:4, :]).astype(BF16)
    mean_ref[...] = mean
    rstd_ref[...] = rstd


def norm_inputs(x, params):
    rows, dim = x.shape
    bm = 256
    row_spec = pl.BlockSpec((bm, dim), lambda i: (i, 0))
    col_spec = pl.BlockSpec((bm, 1), lambda i: (i, 0))
    return pl.pallas_call(
        norm_kernel,
        grid=(rows // bm,),
        in_specs=[row_spec, pl.BlockSpec((4, dim), lambda i: (0, 0))],
        out_specs=[row_spec, row_spec, col_spec, col_spec],
        out_shape=[jax.ShapeDtypeStruct(x.shape, BF16)] * 2 + [jax.ShapeDtypeStruct((rows, 1), F32)] * 2,
        cost_estimate=pl.CostEstimate(flops=rows * dim * 400, bytes_accessed=rows * dim * 6, transcendentals=0),
        compiler_params=params_for(),
        name="norm_inputs",
    )(x, params)


def matmul_kernel(rhs_dim, l_ref, r_ref, o_ref):
    o_ref[...] = dot(l_ref[...], r_ref[...], 1, rhs_dim).astype(BF16)


def matmul(lhs, rhs, rhs_dim, bm, bn):
    rows, depth = lhs.shape
    n = rhs.shape[1 - rhs_dim]
    rhs_spec = pl.BlockSpec((bn, depth), lambda j, i: (j, 0)) if rhs_dim else pl.BlockSpec((depth, bn), lambda j, i: (0, j))
    return pl.pallas_call(
        functools.partial(matmul_kernel, rhs_dim),
        grid=(n // bn, rows // bm),
        in_specs=[pl.BlockSpec((bm, depth), lambda j, i: (i, 0)), rhs_spec],
        out_specs=pl.BlockSpec((bm, bn), lambda j, i: (i, j)),
        out_shape=jax.ShapeDtypeStruct((rows, n), BF16),
        cost_estimate=pl.CostEstimate(flops=2 * rows * depth * n, bytes_accessed=2 * (rows * depth + depth * n + rows * n), transcendentals=0),
        compiler_params=params_for(),
        name="project",
    )(lhs, rhs)


def mlp_kernel(m_ref, dy_ref, up_ref, down_ref, u_ref, dh_ref):
    pre = dot(m_ref[...], up_ref[...], 1, 0)
    act_grad = dot(dy_ref[...], down_ref[...], 1, 1)
    cdf = 0.5 * (1.0 + lax.erf(pre * math.sqrt(0.5)))
    pdf = jnp.exp(-0.5 * pre * pre) * (1.0 / math.sqrt(2.0 * math.pi))
    u_ref[...] = (pre * cdf).astype(BF16)
    dh_ref[...] = (act_grad * (cdf + pre * pdf)).astype(BF16)


def mlp_hidden(m, dy, w_up, w_down):
    rows, dim = m.shape
    ff = w_up.shape[1]
    bm, bn = 256, 1024
    return pl.pallas_call(
        mlp_kernel,
        grid=(ff // bn, rows // bm),
        in_specs=[
            pl.BlockSpec((bm, dim), lambda j, i: (i, 0)),
            pl.BlockSpec((bm, dim), lambda j, i: (i, 0)),
            pl.BlockSpec((dim, bn), lambda j, i: (0, j)),
            pl.BlockSpec((bn, dim), lambda j, i: (j, 0)),
        ],
        out_specs=[pl.BlockSpec((bm, bn), lambda j, i: (i, j))] * 2,
        out_shape=[jax.ShapeDtypeStruct((rows, ff), BF16)] * 2,
        cost_estimate=pl.CostEstimate(flops=4 * rows * dim * ff, bytes_accessed=4 * (rows * dim + dim * ff + rows * ff), transcendentals=rows * ff),
        compiler_params=params_for(),
        name="mlp_hidden",
    )(m, dy, w_up, w_down)


def cot_kernel(dqkv_ref, dh_ref, wq_ref, wu_ref, x_ref, mean_ref, rstd_ref, par_ref, t_ref, ln_ref):
    da = dot(dqkv_ref[...], wq_ref[...], 1, 1)
    dm = dot(dh_ref[...], wu_ref[...], 1, 1)
    xh = (x_ref[...].astype(F32) - mean_ref[...]) * rstd_ref[...]
    t_ref[...] = da * par_ref[0:1, :] + dm * par_ref[2:3, :]
    first = pl.program_id(1) == 0
    for i, value in enumerate([da * xh, da, dm * xh, dm]):
        total = jnp.sum(value, axis=0, keepdims=True)
        ln_ref[i:i + 1, :] = jnp.where(first, total, total + ln_ref[i:i + 1, :])


def cotangents(dqkv, dh, wq, wu, x, mean, rstd, params):
    rows, qkv_width = dqkv.shape
    ff = dh.shape[1]
    dim = x.shape[1]
    bm, bd = 512, 1024
    return pl.pallas_call(
        cot_kernel,
        grid=(dim // bd, rows // bm),
        in_specs=[
            pl.BlockSpec((bm, qkv_width), lambda j, i: (i, 0)),
            pl.BlockSpec((bm, ff), lambda j, i: (i, 0)),
            pl.BlockSpec((bd, qkv_width), lambda j, i: (j, 0)),
            pl.BlockSpec((bd, ff), lambda j, i: (j, 0)),
            pl.BlockSpec((bm, bd), lambda j, i: (i, j)),
            pl.BlockSpec((bm, 1), lambda j, i: (i, 0)),
            pl.BlockSpec((bm, 1), lambda j, i: (i, 0)),
            pl.BlockSpec((4, bd), lambda j, i: (0, j)),
        ],
        out_specs=[pl.BlockSpec((bm, bd), lambda j, i: (i, j)), pl.BlockSpec((4, bd), lambda j, i: (0, j))],
        out_shape=[jax.ShapeDtypeStruct((rows, dim), F32), jax.ShapeDtypeStruct((4, dim), F32)],
        cost_estimate=pl.CostEstimate(flops=2 * rows * dim * (qkv_width + ff), bytes_accessed=rows * dim * 6 + 2 * (qkv_width + ff) * (dim + rows), transcendentals=0),
        compiler_params=params_for(),
        name="cotangents",
    )(dqkv, dh, wq, wu, x, mean, rstd, params)


def wgrad_kernel(count, *refs):
    lhs, rhs, out_ref = refs[:count], refs[count:2 * count], refs[2 * count]
    total = dot(lhs[0][...], rhs[0][...], 0, 0)
    for i in range(1, count):
        total += dot(lhs[i][...], rhs[i][...], 0, 0)
    out_ref[...] = total.astype(BF16)


def weight_grad(lhs, rhs, bm, bn):
    count = len(lhs)
    rows = sum(v.shape[0] for v in lhs)
    m, n = lhs[0].shape[1], rhs[0].shape[1]
    in_specs = [pl.BlockSpec((v.shape[0], bm), lambda j, i: (0, i)) for v in lhs]
    in_specs += [pl.BlockSpec((v.shape[0], bn), lambda j, i: (0, j)) for v in rhs]
    return pl.pallas_call(
        functools.partial(wgrad_kernel, count),
        grid=(n // bn, m // bm),
        in_specs=in_specs,
        out_specs=pl.BlockSpec((bm, bn), lambda j, i: (i, j)),
        out_shape=jax.ShapeDtypeStruct((m, n), BF16),
        cost_estimate=pl.CostEstimate(flops=2 * rows * m * n, bytes_accessed=2 * (rows * (m + n) + m * n), transcendentals=0),
        compiler_params=params_for(),
        name="weight_grad",
    )(*lhs, *rhs)


def norm_stats(x):
    mean = jnp.mean(x, axis=-1, keepdims=True)
    centred = x - mean
    return mean, lax.rsqrt(jnp.mean(centred * centred, axis=-1, keepdims=True) + NORM_EPS)


def solution(mesh):
    act_spec = P('dp', 'tp', None)

    def device_step(layer_in, grad_out, w_qkv, w_out, w_up, w_down, ln_params):
        dim = layer_in.shape[2]
        groups, head_dim = w_qkv.shape[1], w_qkv.shape[3]
        width = groups * head_dim
        wq = jnp.swapaxes(w_qkv, 1, 2).reshape(dim, 3 * width)
        wo = w_out.reshape(width, dim)
        bounds = [sum(SIZES[:i]) for i in range(len(SIZES) + 1)]
        slices = [slice(bounds[i], bounds[i + 1]) for i in range(len(SIZES))]
        gathered = []
        for sl in slices:
            x = lax.all_gather(layer_in[sl], 'tp', axis=1, tiled=True)
            dy = lax.all_gather(grad_out[sl], 'tp', axis=1, tiled=True)
            gathered.append((x, dy))
        seq = gathered[0][0].shape[1]
        cos, sin = rope_tables(seq, head_dim)
        saved = []
        ln_parts = []
        owned = []
        for i, nb in enumerate(SIZES):
            rows = nb * seq
            x, dy = (v.reshape(rows, dim) for v in gathered[i])
            if i:
                x, _ = lax.optimization_barrier((x, ln_parts[-1]))
            a, m, mean, rstd = norm_inputs(x, ln_params)
            qkv = matmul(a, wq, 0, 256, 3 * width)
            dc = matmul(dy, wo, 1, 512, width)
            ctx, dqkv = attention_grads(qkv.reshape(nb, seq, 3 * width), dc.reshape(nb, seq, width), cos, sin, head_dim)
            ctx, dqkv = ctx.reshape(rows, width), dqkv.reshape(rows, 3 * width)
            act, dh = mlp_hidden(m, dy, w_up, w_down)
            cot, ln_part = cotangents(dqkv, dh, wq, w_up, x, mean, rstd, ln_params)
            ln_parts.append(ln_part)
            if i == len(SIZES) - 1:
                grad_ln = lax.psum(sum(ln_parts), 'tp')
            owned.append(lax.psum_scatter(cot.reshape(nb, seq, dim), 'tp', scatter_dimension=1, tiled=True))
            saved.append((a, m, dy, act, dh, ctx, dqkv))
        attn_ins, mlp_ins, grads, acts, hiddens, contexts, qkv_grads = zip(*saved)
        outs = []
        for sl, own in zip(slices, owned):
            x = layer_in[sl].astype(F32)
            mean, rstd = norm_stats(x)
            xh = (x - mean) * rstd
            inner = own - jnp.mean(own, axis=-1, keepdims=True) - xh * jnp.mean(own * xh, axis=-1, keepdims=True)
            outs.append((grad_out[sl].astype(F32) + rstd * inner).astype(BF16))
        grad_in = jnp.concatenate(outs, axis=0)
        grad_qkv = weight_grad(attn_ins, qkv_grads, 512, 1536)
        grad_qkv = jnp.swapaxes(grad_qkv.reshape(dim, 3, groups, head_dim), 1, 2)
        grad_wout = weight_grad(contexts, grads, 512, 1024).reshape(w_out.shape)
        grad_up = weight_grad(mlp_ins, hiddens, 512, 1024)
        grad_down = weight_grad(acts, grads, 512, 1024)
        return grad_in, grad_qkv, grad_wout, grad_up, grad_down, grad_ln

    return jax.shard_map(
        device_step,
        mesh=mesh,
        in_specs=(act_spec, act_spec, P(None, 'tp', None, None), P('tp', None, None, None), P(None, 'tp'), P('tp', None), P(None, None)),
        out_specs=(act_spec, P('dp', 'tp', None, None), P(('dp', 'tp'), None, None, None), P('dp', 'tp'), P(('dp', 'tp'), None), P('dp', None)),
        check_vma=False,
    )
```

```python
import functools
import math

import jax
import jax.numpy as jnp
from jax import lax
from jax.experimental import pallas as pl
from jax.experimental.pallas import tpu as pltpu
from jax.sharding import PartitionSpec as P


NORM_EPS = 1e-5
ROPE_BASE = 10000.0
NEG_BIG = -1e30
SIZES = (4, 6, 6)
VMEM = 63 * 1024 * 1024
F32 = jnp.float32
BF16 = jnp.bfloat16


def dot(lhs, rhs, lc, rc):
    return lax.dot_general(lhs, rhs, (((lc,), (rc,)), ((), ())), preferred_element_type=F32)


def rope_tables(seq_len, head_dim):
    half_dim = head_dim // 2
    inv_freq = ROPE_BASE ** (-2.0 * jnp.arange(half_dim, dtype=F32) / head_dim)
    angles = jnp.arange(seq_len, dtype=F32)[:, None] * inv_freq[None, :]
    sin = jnp.sin(angles)
    cos = jnp.cos(angles)
    return jnp.concatenate([cos, cos], axis=-1), jnp.concatenate([-sin, sin], axis=-1)


def attention_kernel(heads, head_dim, qkv_ref, dc_ref, cos_ref, sin_ref, c_ref, dqkv_ref):
    seq = qkv_ref.shape[1]
    half = head_dim // 2
    width = heads * head_dim
    scale = head_dim ** -0.5
    cos = cos_ref[...]
    sin = sin_ref[...]
    causal = lax.broadcasted_iota(jnp.int32, (seq, seq), 0) >= lax.broadcasted_iota(jnp.int32, (seq, seq), 1)
    each = range(heads)

    def cols(h, kind):
        return slice(kind * width + h * head_dim, kind * width + (h + 1) * head_dim)

    def rope(t):
        return (t * cos + pltpu.roll(t, half, 1) * sin).astype(BF16)

    def rope_back(t):
        return (t * cos - pltpu.roll(t, half, 1) * sin).astype(BF16)

    q2 = [rope(qkv_ref[0, :, cols(h, 0)].astype(F32)) for h in each]
    k2 = [rope(qkv_ref[0, :, cols(h, 1)].astype(F32)) for h in each]
    v = [qkv_ref[0, :, cols(h, 2)] for h in each]
    dc = [dc_ref[0, :, cols(h, 0)] for h in each]
    scores = [dot(q2[h], k2[h], 1, 1) for h in each]
    dpr = [dot(dc[h], v[h], 1, 1) for h in each]
    scores = [jnp.where(causal, t * scale, NEG_BIG) for t in scores]
    weights = [jnp.exp(t - jnp.max(t, axis=-1, keepdims=True)) for t in scores]
    probs = [t * (1.0 / jnp.sum(t, axis=-1, keepdims=True)) for t in weights]
    probs_bf16 = [t.astype(BF16) for t in probs]
    for h in each:
        c_ref[0, :, cols(h, 0)] = dot(probs_bf16[h], v[h], 1, 0).astype(BF16)
    for h in each:
        dqkv_ref[0, :, cols(h, 2)] = dot(probs_bf16[h], dc[h], 0, 0).astype(BF16)
    ds = [(probs[h] * (dpr[h] - jnp.sum(dpr[h] * probs[h], axis=-1, keepdims=True)) * scale).astype(BF16) for h in each]
    for h in each:
        dqkv_ref[0, :, cols(h, 0)] = rope_back(dot(ds[h], k2[h], 1, 0))
    for h in each:
        dqkv_ref[0, :, cols(h, 1)] = rope_back(dot(ds[h], q2[h], 0, 0))


def attention_grads(qkv, dc, cos, sin, head_dim):
    batch, seq, qkv_width = qkv.shape
    width = qkv_width // 3
    heads = width // head_dim
    flops = batch * heads * 6 * 2 * seq * seq * head_dim
    return pl.pallas_call(
        functools.partial(attention_kernel, heads, head_dim),
        grid=(batch,),
        in_specs=[
            pl.BlockSpec((1, seq, qkv_width), lambda b: (b, 0, 0)),
            pl.BlockSpec((1, seq, width), lambda b: (b, 0, 0)),
            pl.BlockSpec((seq, head_dim), lambda b: (0, 0)),
            pl.BlockSpec((seq, head_dim), lambda b: (0, 0)),
        ],
        out_specs=[
            pl.BlockSpec((1, seq, width), lambda b: (b, 0, 0)),
            pl.BlockSpec((1, seq, qkv_width), lambda b: (b, 0, 0)),
        ],
        out_shape=[jax.ShapeDtypeStruct((batch, seq, width), BF16), jax.ShapeDtypeStruct(qkv.shape, BF16)],
        cost_estimate=pl.CostEstimate(flops=flops * 3, bytes_accessed=batch * seq * width * 16, transcendentals=batch * heads * seq * seq),
        compiler_params=params_for(),
        name="attention_grads",
    )(qkv, dc, cos, sin)


def params_for(**kw):
    return pltpu.CompilerParams(vmem_limit_bytes=VMEM, **kw)


def staged(groups, body):
    first = pl.program_id(0) == 0

    @pl.when(first)
    def _():
        for group in groups:
            for copy in group:
                copy.start()
        for n, group in enumerate(groups):
            for copy in group:
                copy.wait()
            body(n)

    @pl.when(jnp.logical_not(first))
    def _():
        for n in range(len(groups)):
            body(n)


def hbm():
    return pl.BlockSpec(memory_space=pl.ANY)


def row_blocks(bm, width):
    return pl.BlockSpec((bm, width), lambda i: (i, 0))


def norm_qkv_kernel(bn, parts, x_ref, w_hbm, par_ref, a_ref, m_ref, mean_ref, rstd_ref, qkv_ref, w_vmem, sem):
    copies = [
        pltpu.make_async_copy(w_hbm.at[:, pl.ds(n * bn, bn)], w_vmem.at[:, pl.ds(n * bn, bn)], sem.at[n])
        for n in range(qkv_ref.shape[1] // bn)
    ]
    first = pl.program_id(0) == 0
    size = x_ref.shape[0] // parts

    def norm(part):
        rows = slice(part * size, (part + 1) * size)
        x = x_ref[rows, :].astype(F32)
        mean = jnp.mean(x, axis=-1, keepdims=True)
        centred = x - mean
        rstd = lax.rsqrt(jnp.mean(centred * centred, axis=-1, keepdims=True) + NORM_EPS)
        xh = centred * rstd
        a_ref[rows, :] = (xh * par_ref[0:1, :] + par_ref[1:2, :]).astype(BF16)
        m_ref[rows, :] = (xh * par_ref[2:3, :] + par_ref[3:4, :]).astype(BF16)
        mean_ref[rows, :] = mean
        rstd_ref[rows, :] = rstd

    @pl.when(first)
    def _():
        for copy in copies:
            copy.start()

    norm(0)

    @pl.when(first)
    def _():
        for copy in copies:
            copy.wait()

    for part in range(parts):
        rows = slice(part * size, (part + 1) * size)
        qkv_ref[rows, :] = dot(a_ref[rows, :], w_vmem[...], 1, 0).astype(BF16)
        if part + 1 < parts:
            norm(part + 1)


def norm_qkv(x, wq, params):
    rows, dim = x.shape
    n = wq.shape[1]
    bm, bn = 256, 512
    return pl.pallas_call(
        functools.partial(norm_qkv_kernel, bn, 2),
        grid=(rows // bm,),
        in_specs=[row_blocks(bm, dim), hbm(), pl.BlockSpec((4, dim), lambda i: (0, 0))],
        out_specs=[row_blocks(bm, dim), row_blocks(bm, dim), row_blocks(bm, 1), row_blocks(bm, 1), row_blocks(bm, n)],
        out_shape=[jax.ShapeDtypeStruct(x.shape, BF16)] * 2 + [jax.ShapeDtypeStruct((rows, 1), F32)] * 2 + [jax.ShapeDtypeStruct((rows, n), BF16)],
        scratch_shapes=[pltpu.VMEM(wq.shape, BF16), pltpu.SemaphoreType.DMA((n // bn,))],
        cost_estimate=pl.CostEstimate(flops=2 * rows * dim * (n + 200), bytes_accessed=rows * dim * 6 + 2 * n * (rows + dim), transcendentals=0),
        compiler_params=params_for(),
        name="norm_qkv",
    )(x, wq, params)


def mlp_kernel(bn, m_ref, dy_ref, up_hbm, down_hbm, out_hbm, u_ref, dh_ref, dc_ref, up_vmem, down_vmem, out_vmem, sem):
    count = u_ref.shape[1] // bn
    piece = [pl.ds(n * bn, bn) for n in range(count)]
    groups = [
        [
            pltpu.make_async_copy(up_hbm.at[:, piece[n]], up_vmem.at[:, piece[n]], sem.at[0, n]),
            pltpu.make_async_copy(down_hbm.at[piece[n], :], down_vmem.at[piece[n], :], sem.at[1, n]),
        ]
        for n in range(count)
    ]
    groups.append([pltpu.make_async_copy(out_hbm, out_vmem, sem.at[0, count])])

    def body(n):
        if n == count:
            dc_ref[...] = dot(dy_ref[...], out_vmem[...], 1, 1).astype(BF16)
            return
        pre = dot(m_ref[...], up_vmem[:, piece[n]], 1, 0)
        act_grad = dot(dy_ref[...], down_vmem[piece[n], :], 1, 1)
        cdf = 0.5 * (1.0 + lax.erf(pre * math.sqrt(0.5)))
        pdf = jnp.exp(-0.5 * pre * pre) * (1.0 / math.sqrt(2.0 * math.pi))
        cols = slice(n * bn, (n + 1) * bn)
        u_ref[:, cols] = (pre * cdf).astype(BF16)
        dh_ref[:, cols] = (act_grad * (cdf + pre * pdf)).astype(BF16)

    staged(groups, body)


def mlp_hidden(m, dy, w_up, w_down, wo):
    rows, dim = m.shape
    ff, width = w_up.shape[1], wo.shape[0]
    bm, bn = 256, 512
    return pl.pallas_call(
        functools.partial(mlp_kernel, bn),
        grid=(rows // bm,),
        in_specs=[row_blocks(bm, dim), row_blocks(bm, dim), hbm(), hbm(), hbm()],
        out_specs=[row_blocks(bm, ff), row_blocks(bm, ff), row_blocks(bm, width)],
        out_shape=[jax.ShapeDtypeStruct((rows, ff), BF16)] * 2 + [jax.ShapeDtypeStruct((rows, width), BF16)],
        scratch_shapes=[
            pltpu.VMEM(w_up.shape, BF16),
            pltpu.VMEM(w_down.shape, BF16),
            pltpu.VMEM(wo.shape, BF16),
            pltpu.SemaphoreType.DMA((2, ff // bn + 1)),
        ],
        cost_estimate=pl.CostEstimate(flops=2 * rows * dim * (2 * ff + width), bytes_accessed=4 * (rows * dim + dim * ff + rows * ff), transcendentals=rows * ff),
        compiler_params=params_for(),
        name="mlp_hidden",
    )(m, dy, w_up, w_down, wo)


def cot_kernel(bd, dqkv_ref, dh_ref, wq_hbm, wu_hbm, x_ref, mean_ref, rstd_ref, par_ref, t_ref, ln_ref, wq_vmem, wu_vmem, sem):
    count = t_ref.shape[1] // bd
    piece = [pl.ds(n * bd, bd) for n in range(count)]
    groups = [
        [
            pltpu.make_async_copy(wq_hbm.at[piece[n], :], wq_vmem.at[piece[n], :], sem.at[0, n]),
            pltpu.make_async_copy(wu_hbm.at[piece[n], :], wu_vmem.at[piece[n], :], sem.at[1, n]),
        ]
        for n in range(count)
    ]

    @pl.when(pl.program_id(0) == 0)
    def _():
        ln_ref[...] = jnp.zeros_like(ln_ref)

    def body(n):
        cols = slice(n * bd, (n + 1) * bd)
        da = dot(dqkv_ref[...], wq_vmem[piece[n], :], 1, 1)
        dm = dot(dh_ref[...], wu_vmem[piece[n], :], 1, 1)
        xh = (x_ref[:, cols].astype(F32) - mean_ref[...]) * rstd_ref[...]
        t_ref[:, cols] = da * par_ref[0:1, cols] + dm * par_ref[2:3, cols]
        for i, value in enumerate([da * xh, da, dm * xh, dm]):
            ln_ref[i:i + 1, cols] += jnp.sum(value, axis=0, keepdims=True)

    staged(groups, body)


def cotangents(dqkv, dh, wq, wu, x, mean, rstd, params):
    rows, qkv_width = dqkv.shape
    ff = dh.shape[1]
    dim = x.shape[1]
    bm, bd = 256, 512
    whole = pl.BlockSpec((4, dim), lambda i: (0, 0))
    return pl.pallas_call(
        functools.partial(cot_kernel, bd),
        grid=(rows // bm,),
        in_specs=[row_blocks(bm, qkv_width), row_blocks(bm, ff), hbm(), hbm(), row_blocks(bm, dim), row_blocks(bm, 1), row_blocks(bm, 1), whole],
        out_specs=[row_blocks(bm, dim), whole],
        out_shape=[jax.ShapeDtypeStruct((rows, dim), F32), jax.ShapeDtypeStruct((4, dim), F32)],
        scratch_shapes=[pltpu.VMEM(wq.shape, BF16), pltpu.VMEM(wu.shape, BF16), pltpu.SemaphoreType.DMA((2, dim // bd))],
        cost_estimate=pl.CostEstimate(flops=2 * rows * dim * (qkv_width + ff), bytes_accessed=rows * dim * 6 + 2 * (qkv_width + ff) * (dim + rows), transcendentals=0),
        compiler_params=params_for(),
        name="cotangents",
    )(dqkv, dh, wq, wu, x, mean, rstd, params)


def chunk_copies(rhs, rhs_vmem, sem, bn):
    offsets = [sum(v.shape[0] for v in rhs[:i]) for i in range(len(rhs))]
    spans = [pl.ds(o, v.shape[0]) for o, v in zip(offsets, rhs)]
    groups = [
        [pltpu.make_async_copy(v.at[:, pl.ds(n * bn, bn)], rhs_vmem.at[span, pl.ds(n * bn, bn)], sem.at[c, n]) for c, (v, span) in enumerate(zip(rhs, spans))]
        for n in range(rhs_vmem.shape[1] // bn)
    ]
    return groups, spans


def wgrad_kernel(count, bn, *refs):
    lhs, rhs = refs[:count], refs[count:2 * count]
    out_ref, rhs_vmem, sem = refs[2 * count:]
    groups, spans = chunk_copies(rhs, rhs_vmem, sem, bn)

    def body(n):
        cols = pl.ds(n * bn, bn)
        total = dot(lhs[0][...], rhs_vmem[spans[0], cols], 0, 0)
        for c in range(1, count):
            total += dot(lhs[c][...], rhs_vmem[spans[c], cols], 0, 0)
        out_ref[:, n * bn:(n + 1) * bn] = total.astype(BF16)

    staged(groups, body)


def weight_grad(lhs, rhs):
    count = len(lhs)
    rows = sum(v.shape[0] for v in lhs)
    m, n = lhs[0].shape[1], rhs[0].shape[1]
    bm, bn = 256, 512
    return pl.pallas_call(
        functools.partial(wgrad_kernel, count, bn),
        grid=(m // bm,),
        in_specs=[pl.BlockSpec((v.shape[0], bm), lambda i: (0, i)) for v in lhs] + [hbm()] * count,
        out_specs=row_blocks(bm, n),
        out_shape=jax.ShapeDtypeStruct((m, n), BF16),
        scratch_shapes=[pltpu.VMEM((rows, n), BF16), pltpu.SemaphoreType.DMA((count, n // bn))],
        cost_estimate=pl.CostEstimate(flops=2 * rows * m * n, bytes_accessed=2 * (rows * (m + n) + m * n), transcendentals=0),
        compiler_params=params_for(),
        name="weight_grad",
    )(*lhs, *rhs)


def wgrad_pair_kernel(count, split, bn, *refs):
    lhs_a, lhs_b, rhs = refs[:count], refs[count:2 * count], refs[2 * count:3 * count]
    out_a, out_b, rhs_vmem, sem = refs[3 * count:]
    groups, spans = chunk_copies(rhs, rhs_vmem, sem, bn)

    def run(lhs, out, n):
        cols = pl.ds(n * bn, bn)
        total = dot(lhs[0][...], rhs_vmem[spans[0], cols], 0, 0)
        for c in range(1, count):
            total += dot(lhs[c][...], rhs_vmem[spans[c], cols], 0, 0)
        out[:, n * bn:(n + 1) * bn] = total.astype(BF16)

    @pl.when(pl.program_id(0) < split)
    def _():
        staged(groups, lambda n: run(lhs_a, out_a, n))

    @pl.when(pl.program_id(0) >= split)
    def _():
        for n in range(len(groups)):
            run(lhs_b, out_b, n)


def weight_grad_pair(lhs_a, lhs_b, rhs):
    count = len(rhs)
    rows = sum(v.shape[0] for v in rhs)
    ma, mb, n = lhs_a[0].shape[1], lhs_b[0].shape[1], rhs[0].shape[1]
    bm, bn = 256, 512
    split, total = ma // bm, (ma + mb) // bm
    at_a = lambda i: jnp.minimum(i, split - 1)
    at_b = lambda i: jnp.maximum(i - split, 0)
    return pl.pallas_call(
        functools.partial(wgrad_pair_kernel, count, split, bn),
        grid=(total,),
        in_specs=[pl.BlockSpec((v.shape[0], bm), lambda i: (0, at_a(i))) for v in lhs_a]
        + [pl.BlockSpec((v.shape[0], bm), lambda i: (0, at_b(i))) for v in lhs_b]
        + [hbm()] * count,
        out_specs=[pl.BlockSpec((bm, n), lambda i: (at_a(i), 0)), pl.BlockSpec((bm, n), lambda i: (at_b(i), 0))],
        out_shape=[jax.ShapeDtypeStruct((ma, n), BF16), jax.ShapeDtypeStruct((mb, n), BF16)],
        scratch_shapes=[pltpu.VMEM((rows, n), BF16), pltpu.SemaphoreType.DMA((count, n // bn))],
        cost_estimate=pl.CostEstimate(flops=2 * rows * (ma + mb) * n, bytes_accessed=2 * (rows * (ma + mb + n) + (ma + mb) * n), transcendentals=0),
        compiler_params=params_for(),
        name="weight_grad_pair",
    )(*lhs_a, *lhs_b, *rhs)


def wgrad_qkv_kernel(count, *refs):
    lhs, rhs = refs[:count], refs[count:2 * count]
    out_ref, rhs_vmem, rows_vmem, sem = refs[2 * count:]
    bm, kinds, heads, head_dim = out_ref.shape
    bn = heads * head_dim
    groups, spans = chunk_copies(rhs, rhs_vmem, sem, bn)

    def body(n):
        cols = pl.ds(n * bn, bn)
        total = dot(lhs[0][...], rhs_vmem[spans[0], cols], 0, 0)
        for c in range(1, count):
            total += dot(lhs[c][...], rhs_vmem[spans[c], cols], 0, 0)
        for h in range(heads):
            rows_vmem[pl.ds(n * heads + h, bm, stride=kinds * heads), :] = total[:, h * head_dim:(h + 1) * head_dim]

    staged(groups, body)
    out_ref[...] = rows_vmem[...].astype(BF16).reshape(out_ref.shape)


def weight_grad_qkv(lhs, rhs, kinds, heads, head_dim):
    count = len(lhs)
    rows = sum(v.shape[0] for v in lhs)
    m, n = lhs[0].shape[1], rhs[0].shape[1]
    bm = 256
    return pl.pallas_call(
        functools.partial(wgrad_qkv_kernel, count),
        grid=(m // bm,),
        in_specs=[pl.BlockSpec((v.shape[0], bm), lambda i: (0, i)) for v in lhs] + [hbm()] * count,
        out_specs=pl.BlockSpec((bm, kinds, heads, head_dim), lambda i: (i, 0, 0, 0)),
        out_shape=jax.ShapeDtypeStruct((m, kinds, heads, head_dim), BF16),
        scratch_shapes=[pltpu.VMEM((rows, n), BF16), pltpu.VMEM((bm * kinds * heads, head_dim), F32), pltpu.SemaphoreType.DMA((count, kinds))],
        cost_estimate=pl.CostEstimate(flops=2 * rows * m * n, bytes_accessed=2 * (rows * (m + n) + m * n), transcendentals=0),
        compiler_params=params_for(),
        name="weight_grad_qkv",
    )(*lhs, *rhs)


def final_kernel(bounds, *refs):
    owned = refs[:-3]
    x_ref, dy_ref, out_ref = refs[-3:]
    step = pl.program_id(0)
    for i, own_ref in enumerate(owned):
        @pl.when(jnp.logical_and(step >= bounds[i], step < bounds[i + 1]))
        def _(own_ref=own_ref):
            x = x_ref[...].astype(F32)
            centred = x - jnp.mean(x, axis=-1, keepdims=True)
            rstd = lax.rsqrt(jnp.mean(centred * centred, axis=-1, keepdims=True) + NORM_EPS)
            xh = centred * rstd
            own = own_ref[...]
            inner = own - jnp.mean(own, axis=-1, keepdims=True) - xh * jnp.mean(own * xh, axis=-1, keepdims=True)
            out_ref[...] = (dy_ref[...].astype(F32) + rstd * inner).astype(BF16)


def input_grad(owned, x, dy, bounds):
    batch, seq, dim = x.shape
    per = math.gcd(*bounds[1:])
    bounds = [b // per for b in bounds]
    block = (per, seq, dim)
    own_specs = [pl.BlockSpec(block, lambda b, lo=bounds[i], hi=bounds[i + 1]: (jnp.clip(b - lo, 0, hi - lo - 1), 0, 0)) for i in range(len(owned))]
    plain = pl.BlockSpec(block, lambda b: (b, 0, 0))
    return pl.pallas_call(
        functools.partial(final_kernel, bounds),
        grid=(batch // per,),
        in_specs=own_specs + [plain, plain],
        out_specs=plain,
        out_shape=jax.ShapeDtypeStruct(x.shape, BF16),
        cost_estimate=pl.CostEstimate(flops=batch * seq * dim * 20, bytes_accessed=batch * seq * dim * 10, transcendentals=0),
        compiler_params=params_for(),
        name="input_grad",
    )(*owned, x, dy)


def butterfly_sum(value, axis, size):
    step = 1
    while step < size:
        value = value + lax.ppermute(value, axis, [(i, i ^ step) for i in range(size)])
        step *= 2
    return value


def solution(mesh):
    act_spec = P('dp', 'tp', None)

    def device_step(layer_in, grad_out, w_qkv, w_out, w_up, w_down, ln_params):
        dim = layer_in.shape[2]
        groups, head_dim = w_qkv.shape[1], w_qkv.shape[3]
        width = groups * head_dim
        wq = jnp.swapaxes(w_qkv, 1, 2).reshape(dim, 3 * width)
        wo = w_out.reshape(width, dim)
        bounds = [sum(SIZES[:i]) for i in range(len(SIZES) + 1)]
        slices = [slice(bounds[i], bounds[i + 1]) for i in range(len(SIZES))]
        gathered = []
        for sl in slices:
            x = lax.all_gather(layer_in[sl], 'tp', axis=1, tiled=True)
            dy = lax.all_gather(grad_out[sl], 'tp', axis=1, tiled=True)
            gathered.append((x, dy))
        seq = gathered[0][0].shape[1]
        cos, sin = rope_tables(seq, head_dim)
        saved = []
        ln_parts = []
        owned = []
        for i, nb in enumerate(SIZES):
            rows = nb * seq
            x, dy = (v.reshape(rows, dim) for v in gathered[i])
            if i:
                x, _ = lax.optimization_barrier((x, ln_parts[-1]))
            a, m, mean, rstd, qkv = norm_qkv(x, wq, ln_params)
            act, dh, dc = mlp_hidden(m, dy, w_up, w_down, wo)
            ctx, dqkv = attention_grads(qkv.reshape(nb, seq, 3 * width), dc.reshape(nb, seq, width), cos, sin, head_dim)
            ctx, dqkv = ctx.reshape(rows, width), dqkv.reshape(rows, 3 * width)
            cot, ln_part = cotangents(dqkv, dh, wq, w_up, x, mean, rstd, ln_params)
            ln_parts.append(ln_part)
            if i == len(SIZES) - 1:
                grad_ln = butterfly_sum(sum(ln_parts), 'tp', mesh.shape['tp'])
            owned.append(lax.psum_scatter(cot.reshape(nb, seq, dim), 'tp', scatter_dimension=1, tiled=True))
            saved.append((a, m, dy, act, dh, ctx, dqkv))
        attn_ins, mlp_ins, grads, acts, hiddens, contexts, qkv_grads = zip(*saved)
        grad_qkv = jnp.swapaxes(weight_grad_qkv(attn_ins, qkv_grads, 3, groups, head_dim), 1, 2)
        grad_up = weight_grad(mlp_ins, hiddens)
        grad_down, grad_wout = weight_grad_pair(acts, contexts, grads)
        grad_wout = grad_wout.reshape(w_out.shape)
        grad_in = input_grad(owned, layer_in, grad_out, bounds)
        return grad_in, grad_qkv, grad_wout, grad_up, grad_down, grad_ln

    return jax.shard_map(
        device_step,
        mesh=mesh,
        in_specs=(act_spec, act_spec, P(None, 'tp', None, None), P('tp', None, None, None), P(None, 'tp'), P('tp', None), P(None, None)),
        out_specs=(act_spec, P('dp', 'tp', None, None), P(('dp', 'tp'), None, None, None), P('dp', 'tp'), P(('dp', 'tp'), None), P('dp', None)),
        check_vma=False,
    )
```
